32 devices in a mesh: blk: 8 (over z, y), sub: 4 (over x, core).
Axes of the slice: x: 2, y: 2, z: 4, core: 2. Of those that a mesh axis runs over, the one named last changes fastest.
Arguments:
- integrals: float32 [32, 4, 32, 6144], P('blk', 'sub'), may hold values from -1 to 1
- slot_order: int32 [32, 4, 32], P('blk', 'sub'), may hold values from 0 to 31, each once within a row
- factor_rows: float32 [32, 4, 32, 4096], P(None, 'sub'), may hold values from -1 to 1.5, as said below
- occ_energy: float32 [384], replicated, may hold values from -1.5 to -0.3
- slab_index: int32 [1], replicated, may hold values from 0 to 127
- virt_energy: float32 [2048], replicated, may hold values from 0.1 to 3
Outputs:
- amplitudes: float32 [6144, 6144], P('blk', 'sub')
The draws below stay inside these ranges and needn't reach their ends.
Inputs may be any that keep to these rules, and one draw needn't show every extreme that they name: `slot_order`: each row of 32 entries holds every number from 0 to 31 once. `factor_rows`: the factor is lower triangular (zero above its diagonal) with diagonal entries between 0.5 and 1.5.
All inputs are finite; a program needn't handle non-finite values.
Results may differ from the reference program's by a relative error of at most 0.0001.
Values sent between devices are 32-bit elements; how exact they have to be, the bound alone decides.
A program may use at most 128 MiB of HBM per device.

```python
import jax
import jax.numpy as jnp
from jax import lax

NAUX = 4096
NVIRT = 2048
NOCC = 3
NOCC_ALL = 384
PIECE = 32
ROUND = 128
ROUNDS = 32
PAIRS = 6144
N_SUB = 4


def draw_factor_rows(key, part):
    diag_key = jax.random.fold_in(key, 11)
    noise_key = jax.random.fold_in(key, 23)
    degrees = 2 * NAUX
    row_ids = jnp.arange(NAUX, dtype=jnp.int32)
    shapes = (degrees - row_ids).astype(jnp.float32) * 0.5
    chi_square = 2.0 * jax.random.gamma(diag_key, shapes, (NAUX,), jnp.float32)
    diagonal = jnp.sqrt(chi_square / jnp.float32(degrees))
    noise = jnp.clip(jax.random.normal(noise_key, (NAUX, NAUX), jnp.float32), -6.0, 6.0)
    row_scale = jnp.ones((NAUX,), jnp.float32)
    below = row_ids[:, None] > row_ids[None, :]
    on_diag = row_ids[:, None] == row_ids[None, :]
    off_part = noise / jnp.sqrt(jnp.float32(degrees))
    diag_part = jnp.clip(diagonal * row_scale, 0.5, 1.5)
    whole = jnp.where(below, off_part, 0.0)
    whole = jnp.where(on_diag, diag_part[:, None], whole)
    return whole.reshape(ROUNDS, ROUND // PIECE, PIECE, NAUX).astype(jnp.float32)


def block_levels(stream_key, shape, shards, low, high):
    def one(dim, blocks):
        steps = jax.random.uniform(jax.random.fold_in(jax.random.fold_in(stream_key, 6), dim), (blocks,), jnp.float32, low / len(shards), high / len(shards))
        return jnp.repeat(jnp.exp(steps), shape[dim] // blocks).reshape((-1,) + (1,) * (len(shape) - dim - 1))

    loudness = one(*shards[0])
    for cut in shards[1:]:
        loudness = loudness * one(*cut)
    return loudness


def centred(own_key, shape, deviation, most, split=(), kind=jnp.bfloat16):
    result = jax.random.normal(own_key, shape, jnp.float32) * deviation
    if len(split) > 0:
        result = block_levels(own_key, shape, split, -0.22, 0.18) * result
    return jnp.clip(result, min=-most, max=most).astype(kind)


def setup_inputs(seed: int = 0) -> dict:
    seeds = jax.random.split(jax.random.key(seed), 7)
    return {
        "integrals": centred(seeds[0], (ROUNDS, N_SUB, PIECE, PAIRS), 0.125, 1.0, ((0, 8), (1, 4)), jnp.float32),
        "slot_order": jax.vmap(lambda own: jax.random.permutation(own, PIECE))(jax.random.split(seeds[1], ROUNDS * N_SUB)).reshape((ROUNDS, N_SUB, PIECE)).astype(jnp.int32),
        "factor_rows": draw_factor_rows(jax.random.fold_in(seeds[6], 71), 0),
        "occ_energy": jnp.clip(jax.random.uniform(seeds[3], (NOCC_ALL,), jnp.float32, -1.5, -0.3), -1.5, -0.3),
        "slab_index": jax.random.randint(seeds[4], (1,), 0, NOCC_ALL // NOCC).astype(jnp.int32),
        "virt_energy": jnp.clip(jax.random.uniform(seeds[5], (NVIRT,), jnp.float32, 0.1, 3.0), 0.1, 3.0),
    }


PRECISE = lax.Precision.HIGHEST

def reference(integrals, slot_order, factor_rows, occ_energy, slab_index, virt_energy):
    piece_len = integrals.shape[2]
    places = jnp.arange(piece_len, dtype=jnp.int32)
    onehot = (slot_order[..., None] == places).astype(jnp.float32)
    canonical = jnp.einsum('rscq,rscp->rsqp', onehot, integrals.astype(jnp.float32), precision=PRECISE)
    right_side = canonical.reshape(NAUX, PAIRS)
    factor = factor_rows.reshape(NAUX, NAUX)
    fitted = jax.scipy.linalg.solve_triangular(factor, right_side, lower=True)
    coulomb = lax.dot_general(fitted, fitted, (((0,), (0,)), ((), ())), precision=PRECISE)
    slab_start = slab_index[0].astype(jnp.int32) * NOCC
    occ_slab = lax.dynamic_slice_in_dim(occ_energy, slab_start, NOCC)
    pair_energy = jnp.repeat(occ_slab, NVIRT) - jnp.tile(virt_energy, NOCC)
    return coulomb / (pair_energy[:, None] + pair_energy[None, :])
```

```python
import jax
import jax.numpy as jnp
from jax import lax
from jax.experimental import pallas as pl
from jax.experimental.pallas import tpu as pltpu
from jax.sharding import PartitionSpec as P

NVIRT = 2048
NOCC = 3

EXACT = lax.Precision.HIGHEST
FAST = lax.Precision.HIGH


def canonical_order(integrals, slot_order):
    piece_len = integrals.shape[2]
    places = jnp.arange(piece_len, dtype=jnp.int32)
    onehot = (slot_order[..., None] == places).astype(jnp.float32)
    return jnp.einsum("rscq,rscp->rsqp", onehot, integrals, precision=EXACT)


def transposed_dot(left, right):
    return lax.dot_general(left, right, (((0,), (0,)), ((), ())), precision=FAST)


def exact_dot(left, right):
    return jnp.dot(left, right, precision=EXACT, preferred_element_type=jnp.float32)


def invert_kernel(factor_ref, inverse_ref):
    size = factor_ref.shape[0]
    base = min(128, size)
    row = lax.broadcasted_iota(jnp.int32, (base, base), 0)
    col = lax.broadcasted_iota(jnp.int32, (base, base), 1)
    inverses = []
    for start in range(0, size, base):
        block = factor_ref[start : start + base, start : start + base]
        inverses.append(jnp.where(row == col, 1.0 / jnp.where(row == col, block, 1.0), 0.0))
    width = 1
    while width < base:
        below = (row // (2 * width) == col // (2 * width)) & (
            (row // width) % 2 == 1
        ) & ((col // width) % 2 == 0)
        for index, start in enumerate(range(0, size, base)):
            block = factor_ref[start : start + base, start : start + base]
            part = jnp.where(below, block, 0.0)
            inverse = inverses[index]
            inverses[index] = inverse - exact_dot(exact_dot(inverse, part), inverse)
        width *= 2
    inverse_ref[...] = jnp.zeros_like(inverse_ref)
    for index, start in enumerate(range(0, size, base)):
        inverse_ref[start : start + base, start : start + base] = inverses[index]
    width = base
    while width < size:
        for start in range(0, size, 2 * width):
            top = slice(start, start + width)
            low = slice(start + width, start + 2 * width)
            inner = exact_dot(inverse_ref[low, low], factor_ref[low, top])
            inverse_ref[low, top] = -exact_dot(inner, inverse_ref[top, top])
        width *= 2


def invert(block):
    return pl.pallas_call(
        invert_kernel,
        out_shape=jax.ShapeDtypeStruct(block.shape, jnp.float32),
        in_specs=[pl.BlockSpec(memory_space=pltpu.VMEM)],
        out_specs=pl.BlockSpec(memory_space=pltpu.VMEM),
        cost_estimate=pl.CostEstimate(
            flops=block.shape[0] ** 3 * 8, bytes_accessed=block.size * 8, transcendentals=0
        ),
    )(block)


def shards(integrals, slot_order, factor_rows, occ_energy, slab_index, virt_energy):
    blk_count = lax.axis_size("blk")
    sub_count = lax.axis_size("sub")
    blk_index = lax.axis_index("blk")
    sub_index = lax.axis_index("sub")
    rounds = factor_rows.shape[0]
    piece_len = factor_rows.shape[2]
    section_count = min(8, rounds)
    per_section = rounds // section_count
    own_len = per_section * piece_len
    width = own_len * sub_count

    canonical = canonical_order(integrals, slot_order)
    local_rhs = lax.all_to_all(canonical, "blk", split_axis=3, concat_axis=0, tiled=True)
    pair_cols = local_rhs.shape[3]
    rhs = local_rhs.reshape(section_count, own_len, pair_cols)
    own_rows = factor_rows.reshape(section_count * own_len, section_count * width)

    per_blk = max(1, section_count // blk_count)
    inverses = []
    for part in range(per_blk):
        section = lax.rem(blk_index * per_blk + part, section_count)
        own_diag = lax.dynamic_slice(
            own_rows, (section * own_len, section * width), (own_len, width)
        )
        diag = lax.all_gather(own_diag, "sub", axis=0, tiled=True)
        diag = diag.reshape(sub_count, per_section, piece_len, width)
        diag = diag.transpose(1, 0, 2, 3).reshape(width, width)
        inverse = invert(diag).reshape(width, per_section, sub_count, piece_len)
        inverses.append(inverse.transpose(0, 2, 1, 3).reshape(width, width))
    inverses = lax.all_gather(jnp.stack(inverses), "blk", axis=0, tiled=True)

    quarter = pair_cols // sub_count
    half = blk_count // 2
    shifts = [
        [(source, (source - shift) % blk_count) for source in range(blk_count)]
        for shift in range(half + 1)
    ]
    chunk_sections = max(1, section_count // 4)
    pieces = [None] * (half + 1)

    updated = rhs[0]
    rest = rhs[1:].reshape((section_count - 1) * own_len, pair_cols)
    chunk = []
    for section in range(section_count):
        gathered = lax.all_gather(updated, "sub", axis=0, tiled=True)
        solved = jnp.dot(inverses[section], gathered, precision=FAST)
        columns = slice(section * width, (section + 1) * width)
        if section + 1 < section_count:
            first = (section + 1) * own_len
            updated = rest[:own_len] - jnp.dot(
                own_rows[first : first + own_len, columns], solved, precision=FAST
            )
        if section + 2 < section_count:
            rest = rest[own_len:] - jnp.dot(
                own_rows[first + own_len :, columns], solved, precision=FAST
            )
        chunk.append(solved)
        if len(chunk) == chunk_sections:
            known = jnp.concatenate(chunk)
            chunk = []
            own_part = lax.dynamic_slice_in_dim(known, sub_index * quarter, quarter, axis=1)
            for shift in range(half + 1):
                moved = lax.ppermute(own_part, "blk", shifts[shift]) if shift else own_part
                term = transposed_dot(moved, known)
                pieces[shift] = term if pieces[shift] is None else pieces[shift] + term

    mirrored = []
    for shift in range(half - 1, 0, -1):
        back = [(target, source) for source, target in shifts[shift]]
        mirrored.append(lax.ppermute(pieces[shift], "blk", back))
    by_offset = jnp.stack(pieces + mirrored)
    by_block = jnp.roll(by_offset, blk_index, axis=0)
    exchanged = lax.all_to_all(by_block, "sub", split_axis=0, concat_axis=1, tiled=True)
    per_sub = blk_count // sub_count
    blocks = exchanged.reshape(per_sub, sub_count * quarter, pair_cols)
    offsets = jnp.mod(sub_index * per_sub + jnp.arange(per_sub) - blk_index, blk_count)
    turned = jnp.where((offsets <= half)[:, None, None], blocks.transpose(0, 2, 1), blocks)
    coulomb = turned.transpose(1, 0, 2).reshape(pair_cols, per_sub * pair_cols)

    slab_start = slab_index[0] * NOCC
    occ_slab = lax.dynamic_slice_in_dim(occ_energy, slab_start, NOCC)
    pair_energy = jnp.repeat(occ_slab, NVIRT) - jnp.tile(virt_energy, NOCC)
    total_quarter = per_sub * pair_cols
    row_energy = lax.dynamic_slice_in_dim(pair_energy, blk_index * pair_cols, pair_cols)
    col_energy = lax.dynamic_slice_in_dim(pair_energy, sub_index * total_quarter, total_quarter)
    return coulomb / (row_energy[:, None] + col_energy[None, :])


def solution(mesh):
    in_specs = (
        P("blk", "sub", None, None),
        P("blk", "sub", None),
        P(None, "sub", None, None),
        P(),
        P(),
        P(),
    )
    out_specs = P("blk", "sub")
    return jax.shard_map(shards, mesh=mesh, in_specs=in_specs, out_specs=out_specs, check_vma=False)
```

```python
import jax
import jax.numpy as jnp
from jax import lax
from jax.experimental import pallas as pl
from jax.experimental.pallas import tpu as pltpu
from jax.sharding import PartitionSpec as P

NVIRT = 2048
NOCC = 3

EXACT = lax.Precision.HIGHEST
FAST = lax.Precision.HIGH


def canonical_order(integrals, slot_order, blk_count):
    rounds, sub, piece_len, total = integrals.shape
    places = jnp.arange(piece_len, dtype=jnp.int32)
    onehot = (slot_order[..., None] == places).astype(jnp.float32)
    ordered = jnp.einsum("rscq,rscp->rsqp", onehot, integrals, precision=EXACT)
    rows = ordered.reshape(rounds * sub * piece_len, total)
    width = total // blk_count
    return jnp.stack([rows[:, i * width : (i + 1) * width] for i in range(blk_count)])


def transposed_dot(left, right):
    return lax.dot_general(left, right, (((0,), (0,)), ((), ())), precision=FAST)


def exact_dot(left, right):
    return jnp.dot(left, right, precision=EXACT, preferred_element_type=jnp.float32)


def invert_kernel(factor_ref, inverse_ref):
    size = factor_ref.shape[0]
    base = min(128, size)
    row = lax.broadcasted_iota(jnp.int32, (base, base), 0)
    col = lax.broadcasted_iota(jnp.int32, (base, base), 1)
    inverses = []
    for start in range(0, size, base):
        block = factor_ref[start : start + base, start : start + base]
        inverses.append(jnp.where(row == col, 1.0 / jnp.where(row == col, block, 1.0), 0.0))
    width = 1
    while width < base:
        below = (row // (2 * width) == col // (2 * width)) & (
            (row // width) % 2 == 1
        ) & ((col // width) % 2 == 0)
        for index, start in enumerate(range(0, size, base)):
            block = factor_ref[start : start + base, start : start + base]
            part = jnp.where(below, block, 0.0)
            inverse = inverses[index]
            inverses[index] = inverse - exact_dot(exact_dot(inverse, part), inverse)
        width *= 2
    inverse_ref[...] = jnp.zeros_like(inverse_ref)
    for index, start in enumerate(range(0, size, base)):
        inverse_ref[start : start + base, start : start + base] = inverses[index]
    width = base
    while width < size:
        for start in range(0, size, 2 * width):
            top = slice(start, start + width)
            low = slice(start + width, start + 2 * width)
            inner = exact_dot(inverse_ref[low, low], factor_ref[low, top])
            inverse_ref[low, top] = -exact_dot(inner, inverse_ref[top, top])
        width *= 2


def invert(block):
    return pl.pallas_call(
        invert_kernel,
        out_shape=jax.ShapeDtypeStruct(block.shape, jnp.float32),
        in_specs=[pl.BlockSpec(memory_space=pltpu.VMEM)],
        out_specs=pl.BlockSpec(memory_space=pltpu.VMEM),
        cost_estimate=pl.CostEstimate(
            flops=block.shape[0] ** 3 * 8, bytes_accessed=block.size * 8, transcendentals=0
        ),
    )(block)


def shards(integrals, slot_order, factor_rows, occ_energy, slab_index, virt_energy):
    blk_count = lax.axis_size("blk")
    sub_count = lax.axis_size("sub")
    blk_index = lax.axis_index("blk")
    sub_index = lax.axis_index("sub")
    rounds = factor_rows.shape[0]
    piece_len = factor_rows.shape[2]
    section_count = min(8, rounds)
    per_section = rounds // section_count
    own_len = per_section * piece_len
    width = own_len * sub_count

    own_rows = factor_rows.reshape(section_count * own_len, section_count * width)
    own_diag = jnp.stack(
        [
            own_rows[i * own_len : (i + 1) * own_len, i * width : (i + 1) * width]
            for i in range(section_count)
        ]
    )
    diag_rows = lax.all_gather(own_diag, "sub", axis=0)

    canonical = canonical_order(integrals, slot_order, blk_count)
    local_rhs = lax.all_to_all(canonical, "blk", split_axis=0, concat_axis=0, tiled=True)
    pair_cols = local_rhs.shape[2]
    rhs = local_rhs.reshape(section_count, own_len, pair_cols)

    def diagonal(section):
        diag = diag_rows[:, section].reshape(sub_count, per_section, piece_len, width)
        return diag.transpose(1, 0, 2, 3).reshape(width, width)

    def inverse_of(diag):
        inverse = invert(diag).reshape(width, per_section, sub_count, piece_len)
        return inverse.transpose(0, 2, 1, 3).reshape(width, width)

    ring = list(range(0, blk_count, 2)) + list(range(blk_count - 1, 0, -2))
    place = [ring.index(i) for i in range(blk_count)]
    places = jnp.array(place, jnp.int32)

    quarter = pair_cols // sub_count
    half = blk_count // 2
    shifts = [
        [(ring[i], ring[(i - shift) % blk_count]) for i in range(blk_count)]
        for shift in range(half + 1)
    ]
    chunk_sections = max(1, section_count // 4)
    pieces = [None] * (half + 1)

    def finish(known, moved):
        for shift in range(half + 1):
            term = transposed_dot(moved[shift], known)
            pieces[shift] = term if pieces[shift] is None else pieces[shift] + term

    updated = rhs[0]
    rest = rhs[1:].reshape((section_count - 1) * own_len, pair_cols)
    chunk = []
    inverse = inverse_of(diagonal(0))
    flying = []
    for section in range(section_count):
        if len(flying) > 1:
            updated, arrived = lax.optimization_barrier((updated, flying.pop(0)))
            finish(*arrived)
        if section + 1 < section_count:
            following, updated = lax.optimization_barrier((diagonal(section + 1), updated))
        gathered = lax.all_gather(updated, "sub", axis=0, tiled=True)
        solved = jnp.dot(inverse, gathered, precision=FAST)
        if section + 1 < section_count:
            inverse = inverse_of(following)
        columns = slice(section * width, (section + 1) * width)
        if section + 1 < section_count:
            first = (section + 1) * own_len
            updated = rest[:own_len] - jnp.dot(
                own_rows[first : first + own_len, columns], solved, precision=FAST
            )
        if section + 2 < section_count:
            rest = rest[own_len:] - jnp.dot(
                own_rows[first + own_len :, columns], solved, precision=FAST
            )
        chunk.append(solved)
        if len(chunk) == chunk_sections:
            known = jnp.concatenate(chunk)
            chunk = []
            own_part = lax.dynamic_slice_in_dim(known, sub_index * quarter, quarter, axis=1)
            moved = [own_part]
            for shift in range(half):
                moved.append(lax.ppermute(moved[-1], "blk", shifts[1]))
            flying.append((known, moved))
    for arrived in flying:
        finish(*arrived)

    mirrored = []
    for shift in range(half - 1, 0, -1):
        back = [(target, source) for source, target in shifts[shift]]
        mirrored.append(lax.ppermute(pieces[shift], "blk", back))
    by_offset = jnp.stack(pieces + mirrored)
    from_here = jnp.mod(places - places[blk_index], blk_count)
    by_block = jnp.stack(
        [lax.dynamic_index_in_dim(by_offset, from_here[i], 0, keepdims=False) for i in range(blk_count)]
    )
    exchanged = lax.all_to_all(by_block, "sub", split_axis=0, concat_axis=1, tiled=True)
    per_sub = blk_count // sub_count
    blocks = exchanged.reshape(per_sub, sub_count * quarter, pair_cols)
    offsets = lax.dynamic_slice_in_dim(from_here, sub_index * per_sub, per_sub)
    turned = jnp.where((offsets <= half)[:, None, None], blocks.transpose(0, 2, 1), blocks)
    coulomb = turned.transpose(1, 0, 2).reshape(pair_cols, per_sub * pair_cols)

    slab_start = slab_index[0] * NOCC
    occ_slab = lax.dynamic_slice_in_dim(occ_energy, slab_start, NOCC)
    pair_energy = jnp.repeat(occ_slab, NVIRT) - jnp.tile(virt_energy, NOCC)
    total_quarter = per_sub * pair_cols
    row_energy = lax.dynamic_slice_in_dim(pair_energy, blk_index * pair_cols, pair_cols)
    col_energy = lax.dynamic_slice_in_dim(pair_energy, sub_index * total_quarter, total_quarter)
    return coulomb / (row_energy[:, None] + col_energy[None, :])


def solution(mesh):
    in_specs = (
        P("blk", "sub", None, None),
        P("blk", "sub", None),
        P(None, "sub", None, None),
        P(),
        P(),
        P(),
    )
    out_specs = P("blk", "sub")
    return jax.shard_map(shards, mesh=mesh, in_specs=in_specs, out_specs=out_specs, check_vma=False)
```
